32 devices in a mesh: grp: 4 (over x, core), tile: 8 (over z, y).
Axes of the slice: x: 2, y: 2, z: 4, core: 2. Of those that a mesh axis runs over, the one named last changes fastest.
Arguments:
- amplitudes: bfloat16 [40, 4, 245760], P(None, None, ('grp', 'tile')), may hold values from -6 to 6
- w_vvvo: bfloat16 [1024, 245760], P(None, ('grp', 'tile')), may hold values from -0.0234375 to 0.0234375
- pair_mask: int32 [1024], P(('grp', 'tile')), may hold values from 0 to 1, as said below
- owner_map: int32 [8], replicated, may hold values from 0 to 7, each once
Outputs:
- sigma_one: float32 [40, 4, 1024], P('tile', None, 'grp')
The draws below stay inside these ranges and needn't reach their ends.
Inputs may be any that keep to these rules, and one draw needn't show every extreme that they name: `pair_mask`: in each aligned block of 32 pairs at most 24 are 1 and at least one is; some block has exactly 24 and some block exactly one. `owner_map`: a permutation of the row blocks.
All inputs are finite; a program needn't handle non-finite values.
Results may differ from the reference program's by a relative error of at most 0.0003.
Values sent between devices are 32-bit elements; how exact they have to be, the bound alone decides.
A program may use at most 128 MiB of HBM per device.

```python
import jax
import jax.numpy as jnp
from jax import lax

V = 1024
O = 240
NR = 4
IROW = 5
PAIR_DEV = 32
LIVE_DEV = 24
I = 40
PAIRS = 1024
N_TILE = 8


def draw_pair_mask(key, part):
    groups = PAIRS // PAIR_DEV
    base = jax.random.fold_in(key, 11)
    key_count, key_full, key_perm = jax.random.split(base, 3)
    counts = jax.random.randint(key_count, (groups,), 1, LIVE_DEV + 1)
    full_group = jax.random.randint(key_full, (), 0, groups)
    sparse_group = (full_group + 1) % groups
    counts = jnp.where(jnp.arange(groups) == full_group, LIVE_DEV, counts)
    counts = jnp.where(jnp.arange(groups) == sparse_group, 1, counts)
    order_ranks = jax.vmap(lambda subkey: jax.random.permutation(subkey, PAIR_DEV))(jax.random.split(key_perm, groups))
    return (order_ranks < counts[:, None]).astype(jnp.int32).reshape(PAIRS)


def with_spikes(result, rng, source, target, blocks, factor):
    owner, partner = [(jnp.arange(result.shape[axis_at]) // (result.shape[axis_at] // blocks)).reshape([-1 if axis == axis_at else 1 for axis in range(result.ndim)]) for axis_at in (source, target)]
    chosen = jax.random.permutation(rng, blocks)[partner]
    strong = (owner == chosen) | (owner == (partner + blocks // 2) % blocks)
    return jnp.where(strong, factor * result, result)


def block_levels(key, dims, shards, low, top_value):
    loudness = 1.0
    for axis_at, parts in shards:
        draws = jax.random.uniform(jax.random.fold_in(jax.random.fold_in(key, 6), axis_at), (parts,), jnp.float32, low / len(shards), top_value / len(shards))
        loudness = loudness * jnp.repeat(jnp.exp(draws), dims[axis_at] // parts).reshape((-1,) + (1,) * (len(dims) - 1 - axis_at))
    return loudness


def centred(own_key, dims, deviation, bound, shards=(), held_as=jnp.bfloat16):
    loudness = block_levels(own_key, dims, shards, -0.22, 0.18) if shards else 1.0
    drawn = jax.random.normal(own_key, dims, jnp.float32) * deviation * loudness
    return jnp.minimum(jnp.maximum(drawn, -bound), bound).astype(held_as)


def noise_with(key, extent, spread, bound, pieces, heavy, held_as=jnp.bfloat16):
    array = spread * jax.random.normal(key, extent, jnp.float32)
    if pieces:
        array = array * block_levels(key, extent, pieces, -0.22, 0.18)
    return jnp.clip(with_spikes(array, jax.random.fold_in(key, 3), *heavy), -bound, bound).astype(held_as)


def setup_inputs(seed: int = 0) -> dict:
    splits = jax.random.split(jax.random.key(seed), 5)
    return {
        "amplitudes": centred(splits[0], (I, NR, PAIRS * O), 1.0, 6.0, ((2, 32),)),
        "w_vvvo": noise_with(splits[1], (V, PAIRS * O), (PAIRS * O) ** -0.5, 0.0234375, ((1, 32),), (1, 0, 32, 2.75)),
        "pair_mask": draw_pair_mask(jax.random.fold_in(splits[4], 71), 0),
        "owner_map": jax.random.permutation(splits[3], N_TILE).astype(jnp.int32),
    }


def reference(amplitudes, w_vvvo, pair_mask, owner_map):
    block_cols = PAIR_DEV * O
    block_total = PAIRS // PAIR_DEV

    def add_block(running, index):
        offset = (index * block_cols).astype(jnp.int32)
        amp_block = lax.dynamic_slice_in_dim(amplitudes, offset, block_cols, 2).astype(jnp.float32)
        mask_part = lax.dynamic_slice_in_dim(pair_mask, (index * PAIR_DEV).astype(jnp.int32), PAIR_DEV, 0)
        mask_cols = jnp.repeat(mask_part.astype(jnp.float32), O)
        w_block = lax.dynamic_slice_in_dim(w_vvvo, offset, block_cols, 1).astype(jnp.float32)
        masked = amp_block * mask_cols
        return running + jnp.einsum("irk,ak->ira", masked, w_block, precision=lax.Precision.HIGHEST), None

    start_value = jnp.zeros((I, NR, V), jnp.float32)
    full_sigma, _ = lax.scan(add_block, start_value, jnp.arange(block_total, dtype=jnp.int32))
    blocked = full_sigma.reshape(N_TILE, IROW, NR, V)
    ordered = jnp.take(blocked, owner_map.astype(jnp.int32), axis=0)
    return ordered.reshape(I, NR, V)
```

```python
import functools

import jax
import jax.numpy as jnp
from jax import lax
from jax.experimental import pallas as pl
from jax.experimental.pallas import tpu as pltpu
from jax.sharding import PartitionSpec as P

MESH = pl.DeviceIdType.MESH
LANES = 128


def chunk_width(total, limit):
    width = limit // LANES * LANES
    while total % width:
        width -= LANES
    return width


def nt_dot(left, right):
    return lax.dot_general(
        left, right, (((1,), (1,)), ((), ())), preferred_element_type=jnp.float32
    )


def mask_row(mask_ref, start, width, occ_width):
    tiles = []
    for tile_start in range(start, start + width, LANES):
        lane = lax.broadcasted_iota(jnp.int32, (8, LANES), 1) + tile_start
        first = tile_start // occ_width
        last = (tile_start + LANES - 1) // occ_width
        row = jnp.full((8, LANES), mask_ref[first], jnp.int32)
        for pair in range(first + 1, last + 1):
            row = jnp.where(lane >= pair * occ_width, mask_ref[pair], row)
        tiles.append(row)
    return jnp.concatenate(tiles, axis=1).astype(jnp.float32)


def kernel(
    planes, tiles, owner_ref, mask_ref, amp_hbm, w_hbm, out_ref,
    amp_raw, amp, keep_row, acc, w_vmem, core_src, core_dst, send_buf, recv_buf,
    amp_sem, w_sem, core_send, core_recv, send_sem, recv_sem,
):
    my_grp = lax.axis_index("grp")
    my_tile = lax.axis_index("tile")
    plane, core = my_grp // 2, my_grp % 2
    occ_total, roots, cols = amp_raw.shape
    occ_rows = occ_total // tiles
    rows = occ_rows * roots
    virt_rows = w_hbm.shape[0] // (2 * planes)
    lane_blocks = virt_rows // LANES
    occ_width = cols // mask_ref.shape[0]
    chunk = chunk_width(cols, 1280)

    def block_of(step):
        there = (plane + planes - 1 - step // 2) % planes
        own = step % 2
        return there * 2 + own * core + (1 - own) * (1 - core)

    def w_copy(step):
        start = pl.multiple_of(block_of(step) * virt_rows, virt_rows)
        return pltpu.make_async_copy(
            w_hbm.at[pl.ds(start, virt_rows)], w_vmem.at[step], w_sem.at[step]
        )

    amp_copy = pltpu.make_async_copy(amp_hbm, amp_raw, amp_sem)
    amp_copy.start()
    for step in range(2 * planes):
        w_copy(step).start()

    barrier = pltpu.get_barrier_semaphore()
    greeted = 0
    pl.semaphore_signal(
        barrier, inc=1, device_id={"grp": my_grp + 1 - 2 * core, "tile": my_tile},
        device_id_type=MESH,
    )
    greeted += 1
    for hop in range(planes):
        for shift in range(tiles):
            if hop or shift:
                pl.semaphore_signal(
                    barrier,
                    inc=1,
                    device_id={
                        "grp": (plane + hop) % planes * 2 + core,
                        "tile": (my_tile + shift) % tiles,
                    },
                    device_id_type=MESH,
                )
                greeted += 1

    for start in range(0, cols, chunk):
        keep_row[:, start : start + chunk] = mask_row(mask_ref, start, chunk, occ_width)

    amp_copy.wait()

    @pl.loop(0, cols // chunk)
    def _(part):
        columns = pl.ds(pl.multiple_of(part * chunk, chunk), chunk)
        keep = keep_row[0:1, columns].astype(jnp.bfloat16)
        for q in range(tiles):
            piece = amp_raw[pl.ds(owner_ref[q] * occ_rows, occ_rows), :, columns]
            amp[q * rows : (q + 1) * rows, columns] = piece.reshape(rows, chunk) * keep

    def core_copy(index):
        return pltpu.make_async_remote_copy(
            src_ref=core_src.at[index],
            dst_ref=core_dst.at[index],
            send_sem=core_send.at[index],
            recv_sem=core_recv.at[index],
            device_id={"grp": my_grp + 1 - 2 * core, "tile": my_tile},
            device_id_type=MESH,
        )

    def piece_copy(hop, target, source):
        return pltpu.make_async_remote_copy(
            src_ref=send_buf.at[hop, target],
            dst_ref=recv_buf.at[hop, source],
            send_sem=send_sem.at[hop, target],
            recv_sem=recv_sem.at[hop, source],
            device_id={"grp": (plane + hop) % planes * 2 + core, "tile": target},
            device_id_type=MESH,
        )

    others = [index + (index >= my_tile).astype(jnp.int32) for index in map(jnp.int32, range(tiles - 1))]

    def each_piece():
        for q in range(tiles):
            for lb in range(lane_blocks):
                yield q, slice(lb * rows, (lb + 1) * rows), acc[
                    q * rows : (q + 1) * rows, lb * LANES : (lb + 1) * LANES
                ]

    @pl.loop(0, 2 * planes)
    def _(step):
        index = step // 2
        hop = planes - 1 - index
        w_copy(step).wait()
        acc[...] = nt_dot(amp[...], w_vmem[step])

        @pl.when(step == 0)
        def _():
            pl.semaphore_wait(barrier, greeted)

        @pl.when(step % 2 == 0)
        def _():
            for q, where, value in each_piece():
                core_src[index, q, where] = value
            core_copy(index).start()

        @pl.when(step % 2 == 1)
        def _():
            core_copy(index).wait_recv()
            for q, where, value in each_piece():
                send_buf[hop, q, where] = value + core_dst[index, q, where]

            @pl.when(hop > 0)
            def _():
                for target in range(tiles):
                    piece_copy(hop, target, my_tile).start()

            @pl.when(hop == 0)
            def _():
                for other in others:
                    piece_copy(hop, other, my_tile).start()

    total = send_buf[0, my_tile]
    pieces = [
        (hop, tile)
        for hop in reversed(range(planes))
        for tile in (range(tiles) if hop else others)
    ]
    for hop, tile in pieces:
        piece_copy(hop, my_tile, tile).wait_recv()
        total = total + recv_buf[hop, tile]
    for lb in range(lane_blocks):
        for i in range(occ_rows):
            at = lb * rows + i * roots
            out_ref[i, :, lb * LANES : (lb + 1) * LANES] = total[at : at + roots]
    for index in range(planes):
        core_copy(index).wait_send()
    for hop, tile in pieces:
        piece_copy(hop, tile, my_tile).wait_send()


def shards(amplitudes, w_vvvo, pair_mask, owner_map):
    occ_total, roots, cols = amplitudes.shape
    virt_total = w_vvvo.shape[0]
    grps, tiles = lax.axis_size("grp"), lax.axis_size("tile")
    planes = grps // 2
    occ_rows = occ_total // tiles
    virt_rows = virt_total // grps
    piece = (virt_rows // LANES * occ_rows * roots, LANES)
    return pl.pallas_call(
        functools.partial(kernel, planes, tiles),
        out_shape=pltpu.VMEM((occ_rows, roots, virt_rows), jnp.float32),
        in_specs=[
            pl.BlockSpec(memory_space=pltpu.SMEM),
            pl.BlockSpec(memory_space=pltpu.SMEM),
            pl.BlockSpec(memory_space=pl.ANY),
            pl.BlockSpec(memory_space=pl.ANY),
        ],
        out_specs=pl.BlockSpec(memory_space=pltpu.VMEM),
        scratch_shapes=[
            pltpu.VMEM((occ_total, roots, cols), jnp.bfloat16),
            pltpu.VMEM((occ_total * roots, cols), jnp.bfloat16),
            pltpu.VMEM((8, cols), jnp.float32),
            pltpu.VMEM((occ_total * roots, virt_rows), jnp.float32),
            pltpu.VMEM((grps, virt_rows, cols), jnp.bfloat16),
            pltpu.VMEM((planes, tiles) + piece, jnp.float32),
            pltpu.VMEM((planes, tiles) + piece, jnp.float32),
            pltpu.VMEM((planes, tiles) + piece, jnp.float32),
            pltpu.VMEM((planes, tiles) + piece, jnp.float32),
            pltpu.SemaphoreType.DMA,
            pltpu.SemaphoreType.DMA((grps,)),
            pltpu.SemaphoreType.DMA((planes,)),
            pltpu.SemaphoreType.DMA((planes,)),
            pltpu.SemaphoreType.DMA((planes, tiles)),
            pltpu.SemaphoreType.DMA((planes, tiles)),
        ],
        compiler_params=pltpu.CompilerParams(
            collective_id=0, has_side_effects=True, vmem_limit_bytes=60 * 1024 * 1024
        ),
        name="sigma",
    )(owner_map, pair_mask, amplitudes, w_vvvo)


def solution(mesh):
    return jax.shard_map(
        shards,
        mesh=mesh,
        in_specs=(
            P(None, None, ("grp", "tile")),
            P(None, ("grp", "tile")),
            P(("grp", "tile")),
            P(),
        ),
        out_specs=P("tile", None, "grp"),
        check_vma=False,
    )
```

```python
import functools

import jax
import jax.numpy as jnp
from jax import lax
from jax.experimental import pallas as pl
from jax.experimental.pallas import tpu as pltpu
from jax.sharding import PartitionSpec as P

MESH = pl.DeviceIdType.MESH
LANES = 128


def chunk_width(total, limit):
    width = limit // LANES * LANES
    while total % width:
        width -= LANES
    return width


def nt_dot(left, right):
    return lax.dot_general(
        left, right, (((1,), (1,)), ((), ())), preferred_element_type=jnp.float32
    )


def mask_row(mask_ref, start, width, occ_width):
    tiles = []
    for tile_start in range(start, start + width, LANES):
        lane = lax.broadcasted_iota(jnp.int32, (8, LANES), 1) + tile_start
        first = tile_start // occ_width
        last = (tile_start + LANES - 1) // occ_width
        row = jnp.full((8, LANES), mask_ref[first], jnp.int32)
        for pair in range(first + 1, last + 1):
            row = jnp.where(lane >= pair * occ_width, mask_ref[pair], row)
        tiles.append(row)
    return jnp.concatenate(tiles, axis=1).astype(jnp.float32)


def kernel(
    planes, tiles, owner_ref, mask_ref, amp_hbm, w_hbm, out_ref,
    amp_raw, amp, keep_row, acc, w_vmem, core_src, core_dst, send_buf, recv_buf,
    amp_sem, w_sem, core_send, core_recv, send_sem, recv_sem,
):
    my_grp = lax.axis_index("grp")
    my_tile = lax.axis_index("tile")
    plane, core = my_grp // 2, my_grp % 2
    occ_total, roots, cols = amp_raw.shape
    occ_rows = occ_total // tiles
    rows = occ_rows * roots
    virt_rows = w_hbm.shape[0] // (2 * planes)
    lane_blocks = virt_rows // LANES
    occ_width = cols // mask_ref.shape[0]
    chunk = chunk_width(cols, 1280)

    def block_of(step):
        there = step // 2
        own = step % 2
        return there * 2 + own * core + (1 - own) * (1 - core)

    def w_copy(step):
        start = pl.multiple_of(block_of(step) * virt_rows, virt_rows)
        return pltpu.make_async_copy(
            w_hbm.at[pl.ds(start, virt_rows)], w_vmem.at[step], w_sem.at[step]
        )

    amp_copy = pltpu.make_async_copy(amp_hbm, amp_raw, amp_sem)
    amp_copy.start()
    for step in range(2 * planes):
        w_copy(step).start()

    barrier = pltpu.get_barrier_semaphore()
    greeted = 0
    pl.semaphore_signal(
        barrier, inc=1, device_id={"grp": my_grp + 1 - 2 * core, "tile": my_tile},
        device_id_type=MESH,
    )
    greeted += 1
    for hop in range(planes):
        for shift in range(tiles):
            if hop or shift:
                pl.semaphore_signal(
                    barrier,
                    inc=1,
                    device_id={
                        "grp": (plane + hop) % planes * 2 + core,
                        "tile": (my_tile + shift) % tiles,
                    },
                    device_id_type=MESH,
                )
                greeted += 1

    for start in range(0, cols, chunk):
        keep_row[:, start : start + chunk] = mask_row(mask_ref, start, chunk, occ_width)

    amp_copy.wait()

    @pl.loop(0, cols // chunk)
    def _(part):
        columns = pl.ds(pl.multiple_of(part * chunk, chunk), chunk)
        keep = keep_row[0:1, columns].astype(jnp.bfloat16)
        for q in range(tiles):
            piece = amp_raw[pl.ds(owner_ref[q] * occ_rows, occ_rows), :, columns]
            amp[q * rows : (q + 1) * rows, columns] = piece.reshape(rows, chunk) * keep

    def core_copy(index):
        return pltpu.make_async_remote_copy(
            src_ref=core_src.at[index],
            dst_ref=core_dst.at[index],
            send_sem=core_send.at[index],
            recv_sem=core_recv.at[index],
            device_id={"grp": my_grp + 1 - 2 * core, "tile": my_tile},
            device_id_type=MESH,
        )

    def piece_copy(hop, target, source):
        return pltpu.make_async_remote_copy(
            src_ref=send_buf.at[hop, target],
            dst_ref=recv_buf.at[hop, source],
            send_sem=send_sem.at[hop, target],
            recv_sem=recv_sem.at[hop, source],
            device_id={"grp": (plane + hop) % planes * 2 + core, "tile": target},
            device_id_type=MESH,
        )

    others = [index + (index >= my_tile).astype(jnp.int32) for index in map(jnp.int32, range(tiles - 1))]

    def each_piece():
        for q in range(tiles):
            for lb in range(lane_blocks):
                yield q, slice(lb * rows, (lb + 1) * rows), acc[
                    q * rows : (q + 1) * rows, lb * LANES : (lb + 1) * LANES
                ]

    @pl.loop(0, 2 * planes)
    def _(step):
        index = step // 2
        hop = (index + planes - plane) % planes
        w_copy(step).wait()
        acc[...] = nt_dot(amp[...], w_vmem[step])

        @pl.when(step == 0)
        def _():
            pl.semaphore_wait(barrier, greeted)

        @pl.when(step % 2 == 0)
        def _():
            for q, where, value in each_piece():
                core_src[index, q, where] = value
            core_copy(index).start()

        @pl.when(step % 2 == 1)
        def _():
            core_copy(index).wait_recv()
            for q, where, value in each_piece():
                send_buf[hop, q, where] = value + core_dst[index, q, where]

            @pl.when(hop > 0)
            def _():
                for target in range(tiles):
                    piece_copy(hop, target, my_tile).start()

            @pl.when(hop == 0)
            def _():
                for other in others:
                    piece_copy(hop, other, my_tile).start()

    total = send_buf[0, my_tile]
    pieces = [
        (hop, tile)
        for hop in reversed(range(planes))
        for tile in (range(tiles) if hop else others)
    ]
    for hop, tile in pieces:
        piece_copy(hop, my_tile, tile).wait_recv()
        total = total + recv_buf[hop, tile]
    for lb in range(lane_blocks):
        for i in range(occ_rows):
            at = lb * rows + i * roots
            out_ref[i, :, lb * LANES : (lb + 1) * LANES] = total[at : at + roots]
    for index in range(planes):
        core_copy(index).wait_send()
    for hop, tile in pieces:
        piece_copy(hop, tile, my_tile).wait_send()


def shards(amplitudes, w_vvvo, pair_mask, owner_map):
    occ_total, roots, cols = amplitudes.shape
    virt_total = w_vvvo.shape[0]
    grps, tiles = lax.axis_size("grp"), lax.axis_size("tile")
    planes = grps // 2
    occ_rows = occ_total // tiles
    virt_rows = virt_total // grps
    piece = (virt_rows // LANES * occ_rows * roots, LANES)
    return pl.pallas_call(
        functools.partial(kernel, planes, tiles),
        out_shape=pltpu.VMEM((occ_rows, roots, virt_rows), jnp.float32),
        in_specs=[
            pl.BlockSpec(memory_space=pltpu.SMEM),
            pl.BlockSpec(memory_space=pltpu.SMEM),
            pl.BlockSpec(memory_space=pl.ANY),
            pl.BlockSpec(memory_space=pl.ANY),
        ],
        out_specs=pl.BlockSpec(memory_space=pltpu.VMEM),
        scratch_shapes=[
            pltpu.VMEM((occ_total, roots, cols), jnp.bfloat16),
            pltpu.VMEM((occ_total * roots, cols), jnp.bfloat16),
            pltpu.VMEM((8, cols), jnp.float32),
            pltpu.VMEM((occ_total * roots, virt_rows), jnp.float32),
            pltpu.VMEM((grps, virt_rows, cols), jnp.bfloat16),
            pltpu.VMEM((planes, tiles) + piece, jnp.float32),
            pltpu.VMEM((planes, tiles) + piece, jnp.float32),
            pltpu.VMEM((planes, tiles) + piece, jnp.float32),
            pltpu.VMEM((planes, tiles) + piece, jnp.float32),
            pltpu.SemaphoreType.DMA,
            pltpu.SemaphoreType.DMA((grps,)),
            pltpu.SemaphoreType.DMA((planes,)),
            pltpu.SemaphoreType.DMA((planes,)),
            pltpu.SemaphoreType.DMA((planes, tiles)),
            pltpu.SemaphoreType.DMA((planes, tiles)),
        ],
        compiler_params=pltpu.CompilerParams(
            collective_id=0, has_side_effects=True, vmem_limit_bytes=60 * 1024 * 1024
        ),
        name="sigma",
    )(owner_map, pair_mask, amplitudes, w_vvvo)


def solution(mesh):
    return jax.shard_map(
        shards,
        mesh=mesh,
        in_specs=(
            P(None, None, ("grp", "tile")),
            P(None, ("grp", "tile")),
            P(("grp", "tile")),
            P(),
        ),
        out_specs=P("tile", None, "grp"),
        check_vma=False,
    )
```

```python
import functools

import jax
import jax.numpy as jnp
from jax import lax
from jax.experimental import pallas as pl
from jax.experimental.pallas import tpu as pltpu
from jax.sharding import PartitionSpec as P

MESH = pl.DeviceIdType.MESH
LANES = 128
MXU = 256


def mask_row(mask_ref, start, width, occ_width):
    tiles = []
    for tile_start in range(start, start + width, LANES):
        lane = lax.broadcasted_iota(jnp.int32, (8, LANES), 1) + tile_start
        first = tile_start // occ_width
        last = (tile_start + LANES - 1) // occ_width
        row = jnp.full((8, LANES), mask_ref[first], jnp.int32)
        for pair in range(first + 1, last + 1):
            row = jnp.where(lane >= pair * occ_width, mask_ref[pair], row)
        tiles.append(row)
    return jnp.concatenate(tiles, axis=1).astype(jnp.float32)


def kernel(
    planes, tiles, owner_ref, mask_ref, amp_hbm, w_hbm, out_ref,
    amp_raw, amp, keep_row, w_vmem, core_src, core_dst, own, send_buf, recv_buf,
    amp_sem, first_sem, w_sem, core_send, core_recv, send_sem, recv_sem,
):
    steps = 2 * planes
    my_grp = lax.axis_index("grp")
    my_tile = lax.axis_index("tile")
    plane, core = my_grp // 2, my_grp % 2
    occ_total, roots, cols = amp_raw.shape
    occ_rows = occ_total // tiles
    rows = occ_rows * roots
    all_rows = occ_total * roots
    virt_rows = w_hbm.shape[0] // steps
    lane_blocks = virt_rows // LANES
    occ_width = cols // mask_ref.shape[0]
    filler = max(0, MXU - all_rows)
    turns = cols // (2 * MXU)
    cut = -(-turns // 2)
    spans = ((0, cut), (cut, turns - cut))

    def block_of(step):
        there = step // 2
        own_half = step % 2
        return there * 2 + own_half * core + (1 - own_half) * (1 - core)

    def rows_of(step):
        return pl.ds(pl.multiple_of(block_of(step) * virt_rows, virt_rows), virt_rows)

    def w_copy(step):
        return pltpu.make_async_copy(w_hbm.at[rows_of(step)], w_vmem.at[step], w_sem.at[step])

    def span_columns(part):
        begin, count = spans[part]
        return pl.ds(begin * 2 * MXU, count * 2 * MXU)

    def first_copy(part):
        where = span_columns(part)
        return pltpu.make_async_copy(
            w_hbm.at[rows_of(0), where], w_vmem.at[0, :, where], first_sem.at[part]
        )

    def amp_copy(part):
        where = span_columns(part)
        return pltpu.make_async_copy(
            amp_hbm.at[:, :, where], amp_raw.at[:, :, where], amp_sem.at[part]
        )

    for part in range(2):
        amp_copy(part).start()
        first_copy(part).start()

    barrier = pltpu.get_barrier_semaphore()
    greeted = 0
    pl.semaphore_signal(
        barrier, inc=1, device_id={"grp": my_grp + 1 - 2 * core, "tile": my_tile},
        device_id_type=MESH,
    )
    greeted += 1
    for hop in range(planes):
        for shift in range(tiles):
            if hop or shift:
                pl.semaphore_signal(
                    barrier,
                    inc=1,
                    device_id={
                        "grp": (plane + hop) % planes * 2 + core,
                        "tile": (my_tile + shift) % tiles,
                    },
                    device_id_type=MESH,
                )
                greeted += 1

    width = 2 * MXU
    for start in range(0, cols, width):
        keep_row[:, start : start + width] = mask_row(mask_ref, start, width, occ_width)

    def masked(part):
        begin, count = spans[part]

        @pl.loop(begin, begin + count)
        def _(index):
            where = pl.ds(pl.multiple_of(index * width, LANES), width)
            keep = keep_row[0:1, where].astype(jnp.bfloat16)
            amp[:, where] = amp_raw[:, :, where].reshape(all_rows, width) * keep

    def core_copy(index):
        return pltpu.make_async_remote_copy(
            src_ref=core_src.at[index],
            dst_ref=core_dst.at[index],
            send_sem=core_send.at[index],
            recv_sem=core_recv.at[index],
            device_id={"grp": my_grp + 1 - 2 * core, "tile": my_tile},
            device_id_type=MESH,
        )

    def piece_copy(hop, target, source):
        return pltpu.make_async_remote_copy(
            src_ref=send_buf.at[hop, target],
            dst_ref=recv_buf.at[hop, source],
            send_sem=send_sem.at[hop, target],
            recv_sem=recv_sem.at[hop, source],
            device_id={"grp": (plane + hop) % planes * 2 + core, "tile": target},
            device_id_type=MESH,
        )

    others = [index + (index >= my_tile).astype(jnp.int32) for index in map(jnp.int32, range(tiles - 1))]

    def blocks(main0, main1, *pads):
        mains = (main0, main1)

        def unit_columns(turn, unit):
            return pl.ds(pl.multiple_of(turn * 2 * MXU + unit * MXU, MXU), MXU)

        def push(step, turn, slot):
            for unit in range(2):
                tile = w_vmem[step, :, unit_columns(turn, unit)]
                pltpu.matmul_push_rhs(tile, slot, unit, transpose=True)

        def multiply(turn, slot):
            for unit in range(2):
                left = amp[:, unit_columns(turn, unit)]
                pltpu.matmul_acc_lhs(mains[unit], left, load_staged_rhs=slot)
                if pads:
                    pltpu.matmul_acc_lhs(pads[unit], jnp.zeros((filler, MXU), jnp.bfloat16))

        def contract(step, begin, turns):
            push(step, begin, 0)

            @pl.loop(0, (turns - 1) // 2)
            def _(trip):
                turn = begin + trip * 2
                push(step, turn + 1, 1)
                multiply(turn, 0)
                push(step, turn + 2, 0)
                multiply(turn + 1, 1)

            if turns % 2:
                multiply(begin + turns - 1, 0)
            else:
                push(step, begin + turns - 1, 1)
                multiply(begin + turns - 2, 0)
                multiply(begin + turns - 1, 1)

        def product():
            return pltpu.matmul_pop(mains[0]) + pltpu.matmul_pop(mains[1])

        def give(index):
            value = product()
            for lb in range(lane_blocks):
                core_src[index, lb] = value[:, lb * LANES : (lb + 1) * LANES]
            core_copy(index).start()

        def scatter(index):
            hop = (index + planes - plane) % planes
            value = product()
            core_copy(index).wait_recv()
            for lb in range(lane_blocks):
                own[lb] = value[:, lb * LANES : (lb + 1) * LANES] + core_dst[index, lb]
            for q in range(tiles):
                source = pl.ds(owner_ref[q] * rows, rows)
                for lb in range(lane_blocks):
                    send_buf[hop, q, lb * rows : (lb + 1) * rows] = own[lb, source]

            @pl.when(hop > 0)
            def _():
                for target in range(tiles):
                    piece_copy(hop, target, my_tile).start()

            @pl.when(hop == 0)
            def _():
                for other in others:
                    piece_copy(hop, other, my_tile).start()

        started = 1
        for part, (begin, count) in enumerate(spans):
            amp_copy(part).wait()
            if started < steps:
                w_copy(started).start()
                started += 1
            masked(part)
            first_copy(part).wait()
            contract(0, begin, count)
        for step in range(started, steps):
            w_copy(step).start()

        pl.semaphore_wait(barrier, greeted)
        give(0)

        @pl.loop(1, steps)
        def _(step):
            w_copy(step).wait()
            contract(step, 0, turns)

            @pl.when(step % 2 == 0)
            def _():
                give(step // 2)

            @pl.when(step % 2 == 1)
            def _():
                scatter(step // 2)

        for pad in pads:
            pltpu.matmul_pop(pad)

    shapes = (all_rows,) + ((filler,) if filler else ())
    pl.run_scoped(
        blocks,
        *(pltpu.ACC(unit)((size, MXU), jnp.float32) for size in shapes for unit in range(2)),
    )

    total = send_buf[0, my_tile]
    pieces = [
        (hop, tile)
        for hop in reversed(range(planes))
        for tile in (range(tiles) if hop else others)
    ]
    for hop, tile in pieces:
        piece_copy(hop, my_tile, tile).wait_recv()
        total = total + recv_buf[hop, tile]
    for lb in range(lane_blocks):
        for i in range(occ_rows):
            at = lb * rows + i * roots
            out_ref[i, :, lb * LANES : (lb + 1) * LANES] = total[at : at + roots]
    for index in range(planes):
        core_copy(index).wait_send()
    for hop, tile in pieces:
        piece_copy(hop, tile, my_tile).wait_send()


def shards(amplitudes, w_vvvo, pair_mask, owner_map):
    occ_total, roots, cols = amplitudes.shape
    virt_total = w_vvvo.shape[0]
    grps, tiles = lax.axis_size("grp"), lax.axis_size("tile")
    planes = grps // 2
    occ_rows = occ_total // tiles
    virt_rows = virt_total // grps
    block = (virt_rows // LANES, occ_total * roots, LANES)
    piece = (virt_rows // LANES * occ_rows * roots, LANES)
    return pl.pallas_call(
        functools.partial(kernel, planes, tiles),
        out_shape=pltpu.VMEM((occ_rows, roots, virt_rows), jnp.float32),
        in_specs=[
            pl.BlockSpec(memory_space=pltpu.SMEM),
            pl.BlockSpec(memory_space=pltpu.SMEM),
            pl.BlockSpec(memory_space=pl.ANY),
            pl.BlockSpec(memory_space=pl.ANY),
        ],
        out_specs=pl.BlockSpec(memory_space=pltpu.VMEM),
        scratch_shapes=[
            pltpu.VMEM((occ_total, roots, cols), jnp.bfloat16),
            pltpu.VMEM((occ_total * roots, cols), jnp.bfloat16),
            pltpu.VMEM((8, cols), jnp.float32),
            pltpu.VMEM((grps, virt_rows, cols), jnp.bfloat16),
            pltpu.VMEM((planes,) + block, jnp.float32),
            pltpu.VMEM((planes,) + block, jnp.float32),
            pltpu.VMEM(block, jnp.float32),
            pltpu.VMEM((planes, tiles) + piece, jnp.float32),
            pltpu.VMEM((planes, tiles) + piece, jnp.float32),
            pltpu.SemaphoreType.DMA((2,)),
            pltpu.SemaphoreType.DMA((2,)),
            pltpu.SemaphoreType.DMA((grps,)),
            pltpu.SemaphoreType.DMA((planes,)),
            pltpu.SemaphoreType.DMA((planes,)),
            pltpu.SemaphoreType.DMA((planes, tiles)),
            pltpu.SemaphoreType.DMA((planes, tiles)),
        ],
        compiler_params=pltpu.CompilerParams(
            collective_id=0, has_side_effects=True, vmem_limit_bytes=60 * 1024 * 1024
        ),
        name="sigma",
    )(owner_map, pair_mask, amplitudes, w_vvvo)


def solution(mesh):
    return jax.shard_map(
        shards,
        mesh=mesh,
        in_specs=(
            P(None, None, ("grp", "tile")),
            P(None, ("grp", "tile")),
            P(("grp", "tile")),
            P(),
        ),
        out_specs=P("tile", None, "grp"),
        check_vma=False,
    )
```

```python
import functools
import math

import jax
import jax.numpy as jnp
from jax import lax
from jax.experimental import pallas as pl
from jax.experimental.pallas import tpu as pltpu
from jax.sharding import PartitionSpec as P

MESH = pl.DeviceIdType.MESH
LANES = 128
MXU = 256


def mask_row(mask_ref, base, width, occ_width):
    tiles = []
    for tile_start in range(0, width, LANES):
        lane = lax.broadcasted_iota(jnp.int32, (8, LANES), 1) + tile_start
        first = tile_start // occ_width
        last = (tile_start + LANES - 1) // occ_width
        row = jnp.full((8, LANES), mask_ref[base + first], jnp.int32)
        for pair in range(first + 1, last + 1):
            row = jnp.where(lane >= pair * occ_width, mask_ref[base + pair], row)
        tiles.append(row)
    return jnp.concatenate(tiles, axis=1).astype(jnp.float32)


def kernel(
    planes, tiles, owner_ref, mask_ref, amp_hbm, w_hbm, out_ref,
    amp_raw, amp, keep_row, w_vmem, core_src, core_dst, own, send_buf, recv_buf,
    amp_sem, first_sem, w_sem, core_send, core_recv, send_sem, recv_sem,
):
    steps = 2 * planes
    my_grp = lax.axis_index("grp")
    my_tile = lax.axis_index("tile")
    plane, core = my_grp // 2, my_grp % 2
    occ_total, roots, cols = amp_raw.shape
    occ_rows = occ_total // tiles
    rows = occ_rows * roots
    all_rows = occ_total * roots
    virt_rows = w_hbm.shape[0] // steps
    lane_blocks = virt_rows // LANES
    occ_width = cols // mask_ref.shape[0]
    filler = max(0, MXU - all_rows)
    turns = cols // (2 * MXU)
    cut = -(-turns // 2)
    spans = ((0, cut), (cut, turns - cut))

    def block_of(step):
        there = step // 2
        own_half = step % 2
        return there * 2 + own_half * core + (1 - own_half) * (1 - core)

    def rows_of(step):
        return pl.ds(pl.multiple_of(block_of(step) * virt_rows, virt_rows), virt_rows)

    def w_copy(step):
        return pltpu.make_async_copy(w_hbm.at[rows_of(step)], w_vmem.at[step], w_sem.at[step])

    def span_columns(part):
        begin, count = spans[part]
        return pl.ds(begin * 2 * MXU, count * 2 * MXU)

    def first_copy(part):
        where = span_columns(part)
        return pltpu.make_async_copy(
            w_hbm.at[rows_of(0), where], w_vmem.at[0, :, where], first_sem.at[part]
        )

    def amp_copy(part):
        where = span_columns(part)
        return pltpu.make_async_copy(
            amp_hbm.at[:, :, where], amp_raw.at[:, :, where], amp_sem.at[part]
        )

    for part in range(2):
        amp_copy(part).start()
        first_copy(part).start()
    w_copy(1).start()

    barrier = pltpu.get_barrier_semaphore()
    greeted = 0
    pl.semaphore_signal(
        barrier, inc=1, device_id={"grp": my_grp + 1 - 2 * core, "tile": my_tile},
        device_id_type=MESH,
    )
    greeted += 1
    @pl.loop(0, tiles)
    def _(other):
        for hop in range(planes):

            @pl.when((hop > 0) | (other != my_tile))
            def _(hop=hop):
                pl.semaphore_signal(
                    barrier,
                    inc=1,
                    device_id={"grp": (plane + hop) % planes * 2 + core, "tile": other},
                    device_id_type=MESH,
                )

    greeted += planes * tiles - 1
    width = 2 * MXU
    period = math.lcm(occ_width, LANES)

    @pl.loop(0, cols // period)
    def _(turn):
        where = pl.ds(pl.multiple_of(turn * period, LANES), period)
        keep_row[:, where] = mask_row(mask_ref, turn * (period // occ_width), period, occ_width)

    def masked(part):
        begin, count = spans[part]

        @pl.loop(begin, begin + count)
        def _(index):
            where = pl.ds(pl.multiple_of(index * width, LANES), width)
            keep = keep_row[0:1, where].astype(jnp.bfloat16)
            amp[:, where] = amp_raw[:, :, where].reshape(all_rows, width) * keep

    def core_copy(index):
        return pltpu.make_async_remote_copy(
            src_ref=core_src.at[index],
            dst_ref=core_dst.at[index],
            send_sem=core_send.at[index],
            recv_sem=core_recv.at[index],
            device_id={"grp": my_grp + 1 - 2 * core, "tile": my_tile},
            device_id_type=MESH,
        )

    def piece_copy(hop, target, source):
        return pltpu.make_async_remote_copy(
            src_ref=send_buf.at[hop, target],
            dst_ref=recv_buf.at[hop, source],
            send_sem=send_sem.at[hop, target],
            recv_sem=recv_sem.at[hop, source],
            device_id={"grp": (plane + hop) % planes * 2 + core, "tile": target},
            device_id_type=MESH,
        )

    others = [index + (index >= my_tile).astype(jnp.int32) for index in map(jnp.int32, range(tiles - 1))]

    def blocks(main0, main1, *pads):
        mains = (main0, main1)

        def unit_columns(turn, unit):
            return pl.ds(pl.multiple_of(turn * 2 * MXU + unit * MXU, MXU), MXU)

        def push(step, turn, slot):
            for unit in range(2):
                tile = w_vmem[step, :, unit_columns(turn, unit)]
                pltpu.matmul_push_rhs(tile, slot, unit, transpose=True)

        def multiply(turn, slot):
            for unit in range(2):
                left = amp[:, unit_columns(turn, unit)]
                pltpu.matmul_acc_lhs(mains[unit], left, load_staged_rhs=slot)
                if pads:
                    pltpu.matmul_acc_lhs(pads[unit], jnp.zeros((filler, MXU), jnp.bfloat16))

        def contract(step, begin, turns):
            push(step, begin, 0)

            @pl.loop(0, (turns - 1) // 2)
            def _(trip):
                turn = begin + trip * 2
                push(step, turn + 1, 1)
                multiply(turn, 0)
                push(step, turn + 2, 0)
                multiply(turn + 1, 1)

            if turns % 2:
                multiply(begin + turns - 1, 0)
            else:
                push(step, begin + turns - 1, 1)
                multiply(begin + turns - 2, 0)
                multiply(begin + turns - 1, 1)

        def product():
            return pltpu.matmul_pop(mains[0]) + pltpu.matmul_pop(mains[1])

        def give(index):
            value = product()
            for lb in range(lane_blocks):
                core_src[index, lb] = value[:, lb * LANES : (lb + 1) * LANES]
            core_copy(index).start()

        def scatter(index):
            hop = (index + planes - plane) % planes
            value = product()
            core_copy(index).wait_recv()
            for lb in range(lane_blocks):
                own[lb] = value[:, lb * LANES : (lb + 1) * LANES] + core_dst[index, lb]
            @pl.loop(0, tiles)
            def _(q):
                source = pl.ds(owner_ref[q] * rows, rows)
                for lb in range(lane_blocks):
                    send_buf[hop, q, lb * rows : (lb + 1) * rows] = own[lb, source]

                @pl.when((hop > 0) | (q != my_tile))
                def _():
                    piece_copy(hop, q, my_tile).start()

        started = 2
        for part, (begin, count) in enumerate(spans):
            amp_copy(part).wait()
            if started < steps:
                w_copy(started).start()
                started += 1
            masked(part)
            first_copy(part).wait()
            contract(0, begin, count)
        for step in range(started, steps):
            w_copy(step).start()

        pl.semaphore_wait(barrier, greeted)
        give(0)

        @pl.loop(1, steps)
        def _(step):
            w_copy(step).wait()
            contract(step, 0, turns)

            @pl.when(step % 2 == 0)
            def _():
                give(step // 2)

            @pl.when(step % 2 == 1)
            def _():
                scatter(step // 2)

        for pad in pads:
            pltpu.matmul_pop(pad)

    shapes = (all_rows,) + ((filler,) if filler else ())
    pl.run_scoped(
        blocks,
        *(pltpu.ACC(unit)((size, MXU), jnp.float32) for size in shapes for unit in range(2)),
    )

    total = send_buf[0, my_tile]
    pieces = [
        (hop, tile)
        for hop in reversed(range(planes))
        for tile in (range(tiles) if hop else others)
    ]
    for hop, tile in pieces:
        piece_copy(hop, my_tile, tile).wait_recv()
        total = total + recv_buf[hop, tile]
    for lb in range(lane_blocks):
        for i in range(occ_rows):
            at = lb * rows + i * roots
            out_ref[i, :, lb * LANES : (lb + 1) * LANES] = total[at : at + roots]
    for index in range(planes):
        core_copy(index).wait_send()
    for hop, tile in pieces:
        piece_copy(hop, tile, my_tile).wait_send()


def shards(amplitudes, w_vvvo, pair_mask, owner_map):
    occ_total, roots, cols = amplitudes.shape
    virt_total = w_vvvo.shape[0]
    grps, tiles = lax.axis_size("grp"), lax.axis_size("tile")
    planes = grps // 2
    occ_rows = occ_total // tiles
    virt_rows = virt_total // grps
    block = (virt_rows // LANES, occ_total * roots, LANES)
    piece = (virt_rows // LANES * occ_rows * roots, LANES)
    return pl.pallas_call(
        functools.partial(kernel, planes, tiles),
        out_shape=pltpu.VMEM((occ_rows, roots, virt_rows), jnp.float32),
        in_specs=[
            pl.BlockSpec(memory_space=pltpu.SMEM),
            pl.BlockSpec(memory_space=pltpu.SMEM),
            pl.BlockSpec(memory_space=pl.ANY),
            pl.BlockSpec(memory_space=pl.ANY),
        ],
        out_specs=pl.BlockSpec(memory_space=pltpu.VMEM),
        scratch_shapes=[
            pltpu.VMEM((occ_total, roots, cols), jnp.bfloat16),
            pltpu.VMEM((occ_total * roots, cols), jnp.bfloat16),
            pltpu.VMEM((8, cols), jnp.float32),
            pltpu.VMEM((grps, virt_rows, cols), jnp.bfloat16),
            pltpu.VMEM((planes,) + block, jnp.float32),
            pltpu.VMEM((planes,) + block, jnp.float32),
            pltpu.VMEM(block, jnp.float32),
            pltpu.VMEM((planes, tiles) + piece, jnp.float32),
            pltpu.VMEM((planes, tiles) + piece, jnp.float32),
            pltpu.SemaphoreType.DMA((2,)),
            pltpu.SemaphoreType.DMA((2,)),
            pltpu.SemaphoreType.DMA((grps,)),
            pltpu.SemaphoreType.DMA((planes,)),
            pltpu.SemaphoreType.DMA((planes,)),
            pltpu.SemaphoreType.DMA((planes, tiles)),
            pltpu.SemaphoreType.DMA((planes, tiles)),
        ],
        compiler_params=pltpu.CompilerParams(
            collective_id=0, has_side_effects=True, vmem_limit_bytes=60 * 1024 * 1024
        ),
        name="sigma",
    )(owner_map, pair_mask, amplitudes, w_vvvo)


def solution(mesh):
    return jax.shard_map(
        shards,
        mesh=mesh,
        in_specs=(
            P(None, None, ("grp", "tile")),
            P(None, ("grp", "tile")),
            P(("grp", "tile")),
            P(),
        ),
        out_specs=P("tile", None, "grp"),
        check_vma=False,
    )
```
